64 devices in a mesh: dp: 4 (over x, y), cp: 16 (over z, core).
Axes of the slice: x: 2, y: 2, z: 8, core: 2. Of those that a mesh axis runs over, the one named last changes fastest.
The devices are a block of a 4x4x8 slice.
Arguments:
- latent: bfloat16 [128, 6, 96, 512], P(('dp', 'cp')), parts along dimension 0
- conv_kernels: bfloat16 [4, 3, 3, 3, 512, 512], replicated
- conv_biases: float32 [4, 512], replicated
- gn_gammas: float32 [4, 512], replicated
- gn_betas: float32 [4, 512], replicated
Outputs:
- output: bfloat16 [128, 6, 96, 512], P(('dp', 'cp')), parts along dimension 0
There are 4 independent parts. The reference program is written for one: setup_inputs(seed, part) draws one part's arguments, and reference() takes and returns one part's arrays. A program takes and returns all parts, laid end to end along the dimension named above; an argument that names none is the same for every part.
All inputs are finite; a program needn't handle non-finite values.
Results may differ from the reference program's by a relative error of at most 0.0126155.
Values are sent between devices in bfloat16 or wider.
A program may use at most 768 MiB of HBM per device.

```python
import jax
import jax.numpy as jnp
from jax import lax

FRAMES = 32
LAT_HEIGHT = 6
LAT_WIDTH = 96
CHANNELS = 512
GROUPS = 32
NORM_EPS = 1e-6


def setup_inputs(seed: int = 0, part: int = 0) -> dict:
    part_key = jax.random.fold_in(jax.random.key(seed), part)
    key_noise, key_slope, key_jitter, key_gain = jax.random.split(part_key, 4)
    key_kernel, key_bias, key_gamma, key_beta = jax.random.split(jax.random.key(seed + 1), 4)
    time_trend = jnp.linspace(-1.0, 1.0, FRAMES)
    chan_slope = jax.random.normal(key_slope, (CHANNELS,))
    frame_mean = time_trend[:, None] * chan_slope[None, :] + 0.3 * jax.random.normal(key_jitter, (FRAMES, CHANNELS))
    frame_gain = jnp.exp(0.5 * time_trend + 0.2 * jax.random.normal(key_gain, (FRAMES,)))
    base_noise = jax.random.normal(key_noise, (FRAMES, LAT_HEIGHT, LAT_WIDTH, CHANNELS))
    latent = base_noise * frame_gain[:, None, None, None] + frame_mean[:, None, None, :]
    conv_kernels = jax.random.normal(key_kernel, (4, 3, 3, 3, CHANNELS, CHANNELS)) * (27 * CHANNELS) ** -0.5
    conv_biases = 0.3 * jax.random.normal(key_bias, (4, CHANNELS))
    gn_gammas = 1.0 + 0.3 * jax.random.normal(key_gamma, (4, CHANNELS))
    gn_betas = 0.3 * jax.random.normal(key_beta, (4, CHANNELS))
    return {"latent": latent.astype(jnp.bfloat16), "conv_kernels": conv_kernels.astype(jnp.bfloat16), "conv_biases": conv_biases.astype(jnp.float32), "gn_gammas": gn_gammas.astype(jnp.float32), "gn_betas": gn_betas.astype(jnp.float32)}


def norm_act(hidden, gn_gamma, gn_beta):
    widened = hidden.astype(jnp.float32)
    grouped = widened.reshape(hidden.shape[:-1] + (GROUPS, CHANNELS // GROUPS))
    elem_count = grouped.size // GROUPS
    sum_one = jnp.sum(grouped, axis=(0, 1, 2, 4))
    sum_sq = jnp.sum(grouped * grouped, axis=(0, 1, 2, 4))
    grp_mean = sum_one / elem_count
    grp_var = sum_sq / elem_count - grp_mean * grp_mean
    normed = (grouped - grp_mean[:, None]) * lax.rsqrt(grp_var + NORM_EPS)[:, None]
    normed = (normed.reshape(hidden.shape) * gn_gamma + gn_beta).astype(jnp.bfloat16)
    return jax.nn.silu(normed.astype(jnp.float32)).astype(jnp.bfloat16)


def causal_conv(act_in, kernel, conv_bias):
    padded = jnp.concatenate([act_in[:1], act_in[:1], act_in], axis=0).astype(jnp.float32)
    result = lax.conv_general_dilated(padded[None], kernel.astype(jnp.float32), (1, 1, 1), ((0, 0), (1, 1), (1, 1)), dimension_numbers=("NDHWC", "DHWIO", "NDHWC"))[0]
    return (result + conv_bias).astype(jnp.bfloat16)


def reference(latent, conv_kernels, conv_biases, gn_gammas, gn_betas):
    def block_step(hidden, block_params):
        kernel_pair, bias_pair, gamma_pair, beta_pair = block_params
        inner = causal_conv(norm_act(hidden, gamma_pair[0], beta_pair[0]), kernel_pair[0], bias_pair[0])
        inner = causal_conv(norm_act(inner, gamma_pair[1], beta_pair[1]), kernel_pair[1], bias_pair[1])
        return (hidden.astype(jnp.float32) + inner.astype(jnp.float32)).astype(jnp.bfloat16), None

    block_params = (conv_kernels.reshape((2, 2) + conv_kernels.shape[1:]), conv_biases.reshape(2, 2, CHANNELS), gn_gammas.reshape(2, 2, CHANNELS), gn_betas.reshape(2, 2, CHANNELS))
    decoded, _ = lax.scan(block_step, latent, block_params)
    return decoded
```

```python
import functools

import jax
import jax.numpy as jnp
from jax import lax
from jax.experimental import pallas as pl
from jax.experimental.pallas import tpu as pltpu
from jax.sharding import PartitionSpec as P

GROUPS = 32
NORM_EPS = 1e-6
F32 = jnp.float32
BF16 = jnp.bfloat16
MESH = pl.DeviceIdType.MESH
TILE = 256
LANES = 128


def _kernel(n_time, n_layers, n_rows, n_cols, n_chans, elem_count,
            x_hbm, w_hbm, bias_ref, gamma_ref, beta_ref, out_hbm,
            raw, xres, act_h0, act_h1, act_a0, act_a1, wbuf, accs, st, ss, stat_tx, stat_rx,
            x_sems, w_sems, halo_send, halo_recv, stat_send, stat_recv, out_sems):
    dp = lax.axis_index("dp")
    me = lax.axis_index("cp")
    acts = (act_h0, act_h1, act_a0, act_a1)
    n_blk = n_chans // LANES
    n_half = n_chans // TILE
    frame_rows = n_rows * n_cols
    group_width = n_chans // GROUPS
    has_next = me < n_time - 1
    has_prev = me > 0
    half_rows = n_rows // 2

    def peer(dist):
        return lax.rem(me + dist, n_time)

    def halo_copy(src, parity, t):
        return pltpu.make_async_remote_copy(
            src_ref=src, dst_ref=raw.at[2 + 2 * parity + t], send_sem=halo_send.at[t],
            recv_sem=halo_recv.at[parity, t], device_id=(dp, lax.rem(me + 1, n_time)), device_id_type=MESH)

    def weight_copy(layer, parity, k):
        return pltpu.make_async_copy(w_hbm.at[layer, k], wbuf.at[parity, k], w_sems.at[parity, k])

    def stat_copy(parity, dist):
        return pltpu.make_async_remote_copy(
            src_ref=stat_tx.at[parity], dst_ref=stat_rx.at[parity, me], send_sem=stat_send.at[parity, dist],
            recv_sem=stat_recv.at[parity, me], device_id=(dp, peer(dist)), device_id_type=MESH)

    def stat_arrival(parity, dist):
        return pltpu.make_async_remote_copy(
            src_ref=stat_tx.at[parity], dst_ref=stat_rx.at[parity, peer(dist)], send_sem=stat_send.at[parity, dist],
            recv_sem=stat_recv.at[parity, peer(dist)], device_id=(dp, peer(dist)), device_id_type=MESH)

    far_first = sorted(range(1, n_time), key=lambda d: -min(d, n_time - d))

    def send_stats(parity):
        for row in range(2):
            total = jnp.sum(st[row], axis=0, keepdims=True)
            for blk in range(n_blk):
                stat_tx[parity, row * n_blk + blk:row * n_blk + blk + 1, :] = total[:, blk * LANES:(blk + 1) * LANES]
        stat_rx[parity, me] = stat_tx[parity]
        for dist in far_first:
            stat_copy(parity, dist).start()

    def finish_stats(layer, parity):
        for dist in range(1, n_time):
            stat_arrival(parity, dist).wait_recv()
        for dist in range(1, n_time):
            stat_copy(parity, dist).wait_send()
        total = stat_rx[parity, 0]
        for src in range(1, n_time):
            total = total + stat_rx[parity, src]
        lane = lax.broadcasted_iota(jnp.int32, total.shape, 1)
        step = 1
        while step < group_width:
            other = jnp.where((lane & step) != 0, pltpu.roll(total, step, 1), pltpu.roll(total, LANES - step, 1))
            total = total + other
            step *= 2
        mean = total[:n_blk] / elem_count
        var = total[n_blk:] / elem_count - mean * mean
        scale = lax.rsqrt(var + NORM_EPS) * gamma_ref[layer]
        shift = beta_ref[layer] - mean * scale
        for blk in range(n_blk):
            ss[0:1, blk * LANES:(blk + 1) * LANES] = scale[blk:blk + 1]
            ss[1:2, blk * LANES:(blk + 1) * LANES] = shift[blk:blk + 1]

    def add_stats(val, lanes):
        grouped = val.reshape(val.shape[0] // 8, 8, val.shape[1])
        st[0, :, lanes] += jnp.sum(grouped, axis=0)
        st[1, :, lanes] += jnp.sum(grouped * grouped, axis=0)

    def norm_item(src_idx, act, row, blk):
        rows = slice(row * n_cols, (row + 1) * n_cols)
        lanes = slice(blk * LANES, (blk + 1) * LANES)
        val = raw[src_idx, rows, lanes].astype(F32)
        val = (val * ss[0:1, lanes] + ss[1:2, lanes]).astype(BF16).astype(F32)
        val = val * lax.logistic(val)
        col = lax.broadcasted_iota(jnp.int32, val.shape, 0)
        act[rows, n_chans + blk * LANES:n_chans + (blk + 1) * LANES] = val.astype(BF16)
        before = jnp.where(col == 0, 0.0, pltpu.roll(val, 1, 0))
        act[rows, blk * LANES:(blk + 1) * LANES] = before.astype(BF16)
        after = jnp.where(col == n_cols - 1, 0.0, pltpu.roll(val, n_cols - 1, 0))
        act[rows, 2 * n_chans + blk * LANES:2 * n_chans + (blk + 1) * LANES] = after.astype(BF16)

    def norm_items(src_idx, act, blks):
        return [functools.partial(norm_item, src_idx, act, row, blk) for blk in blks for row in range(n_rows)]

    def run_body(accs):
        def pop_item(layer, odd, t, row, q):
            rows = slice(row * n_cols, (row + 1) * n_cols)
            lanes = slice(q * TILE, (q + 1) * TILE)
            val = accs[t, rows, lanes] + bias_ref[layer, 0:1, lanes]
            val = val.astype(BF16).astype(F32)
            val = val + xres[0, t, rows, lanes].astype(F32) * odd.astype(F32)
            val = val.astype(BF16)
            raw[t, rows, lanes] = val
            xres[1 - odd, t, rows, lanes] = val
            add_stats(val.astype(F32), lanes)

        def group(parity, k, act, t, rows, first, items):
            lo, hi = rows[0], rows[-1] + 1
            done = 0
            parts = {}
            for idx, di in enumerate((0, -1, 1)):
                r0, r1 = max(lo, -di), min(hi, n_rows - di)
                weight = wbuf[parity, k, (di + 1) * 3 * n_chans:(di + 2) * 3 * n_chans, :]
                prod = jnp.dot(act[(r0 + di) * n_cols:(r1 + di) * n_cols, :], weight, preferred_element_type=F32)
                for row in range(r0, r1):
                    piece = prod[(row - r0) * n_cols:(row - r0 + 1) * n_cols]
                    parts[row] = piece if row not in parts else parts[row] + piece
                upto = (len(items) * (idx + 1)) // 3
                for item in items[done:upto]:
                    item()
                done = upto
            for row in range(lo, hi):
                here = slice(row * n_cols, (row + 1) * n_cols)
                if first:
                    accs[t, here, :] = parts[row]
                else:
                    accs[t, here, :] += parts[row]

        whole = range(n_rows)

        def pops(layer, odd, t, rows):
            return [functools.partial(pop_item, layer, odd, t, row, q) for row in rows for q in range(n_half)]

        barrier = pltpu.get_barrier_semaphore()
        for dist in range(1, n_time):
            pl.semaphore_signal(barrier, inc=1, device_id=(dp, peer(dist)), device_id_type=MESH)
        for t in (1, 0):
            pltpu.make_async_copy(x_hbm.at[t], raw.at[t], x_sems.at[t]).start()
        for k in (2, 1, 0):
            weight_copy(0, 0, k).start()
        for t in (1, 0):
            pltpu.make_async_copy(x_hbm.at[t], xres.at[0, t], x_sems.at[2 + t]).start()
        st[...] = jnp.zeros_like(st)
        for t in (1, 0):
            pltpu.make_async_copy(x_hbm.at[t], raw.at[t], x_sems.at[t]).wait()

            def stat_rows(i, carry, t=t):
                base = pl.multiple_of(i * n_cols, n_cols)
                for q in range(n_half):
                    lanes = slice(q * TILE, (q + 1) * TILE)
                    add_stats(raw[t, pl.ds(base, n_cols), lanes].astype(F32), lanes)
                return carry

            lax.fori_loop(0, n_rows, stat_rows, 0)
        pl.semaphore_wait(barrier, n_time - 1)
        send_stats(0)

        @pl.when(has_next)
        def _():
            for t in (1, 0):
                halo_copy(x_hbm.at[t], 0, t).start()

        def layer_step(layer, carry):
            parity = lax.rem(layer, 2)
            odd = parity
            nxt = 1 - parity
            more = layer < n_layers - 1

            @pl.when(more)
            def _():
                for k in (2, 1, 0):
                    weight_copy(layer + 1, nxt, k).start()

            finish_stats(layer, parity)
            st[...] = jnp.zeros_like(st)
            first_half = range(n_blk // 2)
            second_half = range(n_blk // 2, n_blk)
            for item in norm_items(1, act_a1, first_half):
                item()
            weight_copy(layer, parity, 2).wait()
            for item in norm_items(1, act_a1, second_half):
                item()
            group(parity, 2, act_a1, 1, whole, True, norm_items(0, act_a0, range(n_blk)))

            weight_copy(layer, parity, 1).wait()

            @pl.when(has_prev)
            def _():
                halo_copy(raw.at[1], parity, 1).wait_recv()

            src1 = jnp.where(has_prev, 3 + 2 * parity, 0)
            src0 = jnp.where(has_prev, 2 + 2 * parity, 0)
            group(parity, 1, act_a0, 1, whole, False, norm_items(src1, act_h1, range(n_blk)))

            weight_copy(layer, parity, 0).wait()

            @pl.when(has_next)
            def _():
                halo_copy(raw.at[1], nxt, 1).wait_send()

            @pl.when(layer == 0)
            def _():
                for t in (1, 0):
                    pltpu.make_async_copy(x_hbm.at[t], xres.at[0, t], x_sems.at[2 + t]).wait()

            group(parity, 0, act_h1, 1, whole, False, [])

            @pl.when(has_prev)
            def _():
                halo_copy(raw.at[0], parity, 0).wait_recv()

            for item in pops(layer, odd, 1, whole):
                item()

            @pl.when(jnp.logical_and(more, has_next))
            def _():
                halo_copy(raw.at[1], nxt, 1).start()

            @pl.when(jnp.logical_not(more))
            def _():
                pltpu.make_async_copy(raw.at[1], out_hbm.at[1], out_sems.at[1]).start()

            group(parity, 2, act_a0, 0, whole, True, norm_items(src0, act_h0, range(n_blk)))
            group(parity, 1, act_h1, 0, whole, False, [])

            @pl.when(has_next)
            def _():
                halo_copy(raw.at[0], nxt, 0).wait_send()

            group(parity, 0, act_h0, 0, whole, False, [])
            for item in pops(layer, odd, 0, whole):
                item()

            @pl.when(more)
            def _():
                send_stats(nxt)

            @pl.when(jnp.logical_and(more, has_next))
            def _():
                halo_copy(raw.at[0], nxt, 0).start()

            @pl.when(jnp.logical_not(more))
            def _():
                pltpu.make_async_copy(raw.at[0], out_hbm.at[0], out_sems.at[0]).start()

            return carry

        lax.fori_loop(0, n_layers, layer_step, 0)
        for t in (1, 0):
            pltpu.make_async_copy(raw.at[t], out_hbm.at[t], out_sems.at[t]).wait()

    run_body(accs)


def solution(mesh):
    n_time = mesh.shape["cp"]
    frame_spec = P(("dp", "cp"))

    def local_fn(latent, conv_kernels, conv_biases, gn_gammas, gn_betas):
        n_frames, n_rows, n_cols, n_chans = latent.shape
        n_layers = conv_kernels.shape[0]
        n_taps = conv_kernels.shape[1]
        n_blk = n_chans // LANES
        elem_count = n_time * n_frames * n_rows * n_cols * (n_chans // GROUPS)
        frame = (n_rows * n_cols, n_chans)
        any_spec = pl.BlockSpec(memory_space=pl.ANY)
        vmem_spec = pl.BlockSpec(memory_space=pltpu.VMEM)
        decoded = pl.pallas_call(
            functools.partial(_kernel, n_time, n_layers, n_rows, n_cols, n_chans, float(elem_count)),
            out_shape=jax.ShapeDtypeStruct((n_frames,) + frame, BF16),
            in_specs=[any_spec, any_spec, vmem_spec, vmem_spec, vmem_spec],
            out_specs=any_spec,
            scratch_shapes=[
                pltpu.VMEM((6,) + frame, BF16),
                pltpu.VMEM((2, n_frames) + frame, BF16),
                pltpu.VMEM((frame[0], 3 * n_chans), BF16),
                pltpu.VMEM((frame[0], 3 * n_chans), BF16),
                pltpu.VMEM((frame[0], 3 * n_chans), BF16),
                pltpu.VMEM((frame[0], 3 * n_chans), BF16),
                pltpu.VMEM((2, n_taps, 9 * n_chans, n_chans), BF16),
                pltpu.VMEM((n_frames,) + frame, F32),
                pltpu.VMEM((2, 8, n_chans), F32),
                pltpu.VMEM((8, n_chans), F32),
                pltpu.VMEM((2, 8, LANES), F32),
                pltpu.VMEM((2, n_time, 8, LANES), F32),
                pltpu.SemaphoreType.DMA((4,)),
                pltpu.SemaphoreType.DMA((2, n_taps)),
                pltpu.SemaphoreType.DMA((2,)),
                pltpu.SemaphoreType.DMA((2, 2)),
                pltpu.SemaphoreType.DMA((2, n_time)),
                pltpu.SemaphoreType.DMA((2, n_time)),
                pltpu.SemaphoreType.DMA((2,)),
            ],
            compiler_params=pltpu.CompilerParams(collective_id=0, has_side_effects=True, vmem_limit_bytes=60 * 1024 * 1024),
            name="decoder_blocks",
        )(latent.reshape((n_frames,) + frame), conv_kernels.reshape(n_layers, n_taps, 9 * n_chans, n_chans),
          conv_biases.reshape(n_layers, 1, n_chans), gn_gammas.reshape(n_layers, n_blk, LANES),
          gn_betas.reshape(n_layers, n_blk, LANES))
        return decoded.reshape(latent.shape)

    return jax.shard_map(local_fn, mesh=mesh, in_specs=(frame_spec, P(), P(), P(), P()), out_specs=frame_spec, check_vma=False)
```

```python
import functools

import jax
import jax.numpy as jnp
from jax import lax
from jax.experimental import pallas as pl
from jax.experimental.pallas import tpu as pltpu
from jax.sharding import PartitionSpec as P

GROUPS = 32
NORM_EPS = 1e-6
F32 = jnp.float32
BF16 = jnp.bfloat16
MESH = pl.DeviceIdType.MESH
TILE = 256
LANES = 128


def _kernel(n_time, n_layers, n_rows, n_cols, n_chans, elem_count,
            x_hbm, w_hbm, bias_hbm, gamma_hbm, beta_hbm, out_hbm,
            raw, xres, act_h0, act_h1, act_a0, act_a1, wbuf, accs, st, ss, stat_tx, stat_rx,
            params_in, bias_ref, gamma_ref, beta_ref, x_sems, p_sems, w_sems, halo_send, halo_recv, stat_send, stat_recv, out_sems):
    dp = lax.axis_index("dp")
    me = lax.axis_index("cp")
    acts = (act_h0, act_h1, act_a0, act_a1)
    n_blk = n_chans // LANES
    n_half = n_chans // TILE
    frame_rows = n_rows * n_cols
    group_width = n_chans // GROUPS
    has_next = me < n_time - 1
    has_prev = me > 0
    half_rows = n_rows // 2

    def peer(dist):
        return lax.rem(me + dist, n_time)

    def halo_copy(src, parity, t):
        return pltpu.make_async_remote_copy(
            src_ref=src, dst_ref=raw.at[2 + 2 * parity + t], send_sem=halo_send.at[t],
            recv_sem=halo_recv.at[parity, t], device_id=(dp, lax.rem(me + 1, n_time)), device_id_type=MESH)

    def weight_copy(layer, parity, k):
        return pltpu.make_async_copy(w_hbm.at[layer, k], wbuf.at[parity, k], w_sems.at[parity, k])

    def stat_copy(parity, dist):
        return pltpu.make_async_remote_copy(
            src_ref=stat_tx.at[parity], dst_ref=stat_rx.at[parity, me], send_sem=stat_send.at[parity, dist],
            recv_sem=stat_recv.at[parity, me], device_id=(dp, peer(dist)), device_id_type=MESH)

    def stat_arrival(parity, dist):
        return pltpu.make_async_remote_copy(
            src_ref=stat_tx.at[parity], dst_ref=stat_rx.at[parity, peer(dist)], send_sem=stat_send.at[parity, dist],
            recv_sem=stat_recv.at[parity, peer(dist)], device_id=(dp, peer(dist)), device_id_type=MESH)

    far_first = sorted(range(1, n_time), key=lambda d: -min(d, n_time - d))

    def send_stats(parity):
        for row in range(2):
            total = jnp.sum(st[row], axis=0, keepdims=True)
            for blk in range(n_blk):
                stat_tx[parity, row * n_blk + blk:row * n_blk + blk + 1, :] = total[:, blk * LANES:(blk + 1) * LANES]
        stat_rx[parity, me] = stat_tx[parity]
        for dist in far_first:
            stat_copy(parity, dist).start()

    def finish_stats(layer, parity):
        for dist in range(1, n_time):
            stat_arrival(parity, dist).wait_recv()
        total = stat_rx[parity, 0]
        for src in range(1, n_time):
            total = total + stat_rx[parity, src]
        lane = lax.broadcasted_iota(jnp.int32, total.shape, 1)
        step = 1
        while step < group_width:
            other = jnp.where((lane & step) != 0, pltpu.roll(total, step, 1), pltpu.roll(total, LANES - step, 1))
            total = total + other
            step *= 2
        mean = total[:n_blk] / elem_count
        var = total[n_blk:] / elem_count - mean * mean
        rstd = lax.rsqrt(var + NORM_EPS)
        for blk in range(n_blk):
            lanes = slice(blk * LANES, (blk + 1) * LANES)
            scale = rstd[blk:blk + 1] * gamma_ref[layer, :, lanes]
            ss[0:1, lanes] = scale
            ss[1:2, lanes] = beta_ref[layer, :, lanes] - mean[blk:blk + 1] * scale

    def add_stats(val, lanes):
        grouped = val.reshape(val.shape[0] // 8, 8, val.shape[1])
        st[0, :, lanes] += jnp.sum(grouped, axis=0)
        st[1, :, lanes] += jnp.sum(grouped * grouped, axis=0)

    def norm_item(src_idx, act, row, blk):
        rows = slice(row * n_cols, (row + 1) * n_cols)
        lanes = slice(blk * LANES, (blk + 1) * LANES)
        val = raw[src_idx, rows, lanes].astype(F32)
        val = (val * ss[0:1, lanes] + ss[1:2, lanes]).astype(BF16).astype(F32)
        val = val * lax.logistic(val)
        col = lax.broadcasted_iota(jnp.int32, val.shape, 0)
        act[rows, n_chans + blk * LANES:n_chans + (blk + 1) * LANES] = val.astype(BF16)
        before = jnp.where(col == 0, 0.0, pltpu.roll(val, 1, 0))
        act[rows, blk * LANES:(blk + 1) * LANES] = before.astype(BF16)
        after = jnp.where(col == n_cols - 1, 0.0, pltpu.roll(val, n_cols - 1, 0))
        act[rows, 2 * n_chans + blk * LANES:2 * n_chans + (blk + 1) * LANES] = after.astype(BF16)

    def norm_items(src_idx, act, blks):
        return [functools.partial(norm_item, src_idx, act, row, blk) for blk in blks for row in range(n_rows)]

    def run_body(accs):
        def pop_item(layer, odd, t, row, q):
            rows = slice(row * n_cols, (row + 1) * n_cols)
            lanes = slice(q * TILE, (q + 1) * TILE)
            val = accs[t, rows, lanes] + bias_ref[layer, :, lanes]
            val = val.astype(BF16).astype(F32)
            val = val + xres[0, t, rows, lanes].astype(F32) * odd.astype(F32)
            val = val.astype(BF16)
            raw[t, rows, lanes] = val
            xres[1 - odd, t, rows, lanes] = val
            add_stats(val.astype(F32), lanes)

        def products(parity, steps, rows, items, parts=None):
            lo, hi = rows[0], rows[-1] + 1
            done = 0
            parts = dict(parts or {})
            for idx, (k, act, di, chan, width) in enumerate(steps):
                r0, r1 = max(lo, -di), min(hi, n_rows - di)
                rows_in = slice((r0 + di) * n_cols, (r1 + di) * n_cols)
                base = (di + 1) * 3 * n_chans
                prod = None
                if width == n_chans:
                    prod = jnp.dot(act[rows_in, :], wbuf[parity, k, base:base + 3 * n_chans, :], preferred_element_type=F32)
                else:
                    for dj in range(3):
                        at = dj * n_chans + chan
                        term = jnp.dot(act[rows_in, at:at + width], wbuf[parity, k, base + at:base + at + width, :],
                                       preferred_element_type=F32)
                        prod = term if prod is None else prod + term
                for row in range(r0, r1):
                    piece = prod[(row - r0) * n_cols:(row - r0 + 1) * n_cols]
                    parts[row] = piece if row not in parts else parts[row] + piece
                upto = (len(items) * (idx + 1)) // len(steps)
                for item in items[done:upto]:
                    item()
                done = upto
            return parts

        def tap(k, act, row_taps=(0, -1, 1)):
            return [(k, act, di, 0, n_chans) for di in row_taps]

        def tap_halves(k, act):
            return [(k, act, di, chan, n_chans // 2) for chan in (0, n_chans // 2) for di in (0, -1, 1)]

        def put(t, parts):
            for row, part in parts.items():
                accs[t, row * n_cols:(row + 1) * n_cols, :] = part

        def add(t, parts):
            for row, part in parts.items():
                accs[t, row * n_cols:(row + 1) * n_cols, :] += part

        whole = range(n_rows)
        top = range(half_rows)
        low = range(half_rows, n_rows)

        def pops(layer, odd, t, rows):
            return [functools.partial(pop_item, layer, odd, t, row, q) for row in rows for q in range(n_half)]

        barrier = pltpu.get_barrier_semaphore()
        for dist in range(1, n_time):
            pl.semaphore_signal(barrier, inc=1, device_id=(dp, peer(dist)), device_id_type=MESH)
        for t in (1, 0):
            pltpu.make_async_copy(x_hbm.at[t], raw.at[t], x_sems.at[t]).start()
        params = [pltpu.make_async_copy(src, params_in.at[i], p_sems.at[i])
                  for i, src in enumerate((bias_hbm, gamma_hbm, beta_hbm))]
        for copy in params:
            copy.start()
        for k in (2, 1, 0):
            weight_copy(0, 0, k).start()
        for t in (1, 0):
            pltpu.make_async_copy(x_hbm.at[t], xres.at[0, t], x_sems.at[2 + t]).start()
        st[...] = jnp.zeros_like(st)
        for t in (1, 0):
            pltpu.make_async_copy(x_hbm.at[t], raw.at[t], x_sems.at[t]).wait()

            def stat_rows(i, carry, t=t):
                base = pl.multiple_of(i * n_cols, n_cols)
                for q in range(n_half):
                    lanes = slice(q * TILE, (q + 1) * TILE)
                    add_stats(raw[t, pl.ds(base, n_cols), lanes].astype(F32), lanes)
                return carry

            lax.fori_loop(0, n_rows, stat_rows, 0)
        pl.semaphore_wait(barrier, n_time - 1)
        send_stats(0)

        @pl.when(has_next)
        def _():
            halo_copy(raw.at[1], 0, 1).start()

        for i, (copy, dst) in enumerate(zip(params, (bias_ref, gamma_ref, beta_ref))):
            copy.wait()
            for layer in range(n_layers):
                dst[layer] = params_in[i, layer:layer + 1, :]

        def layer_step(layer, carry):
            parity = lax.rem(layer, 2)
            odd = parity
            nxt = 1 - parity
            more = layer < n_layers - 1

            @pl.when(more)
            def _():
                for k in (2, 1, 0):
                    weight_copy(layer + 1, nxt, k).start()

            finish_stats(layer, parity)

            @pl.when(has_next)
            def _():
                halo_copy(raw.at[0], parity, 0).start()

            st[...] = jnp.zeros_like(st)
            early = range(n_blk // 2)
            late = range(n_blk // 2, n_blk)
            for item in norm_items(1, act_a1, early):
                item()
            weight_copy(layer, parity, 2).wait()
            steps = tap_halves(2, act_a1)
            parts = products(parity, steps[:3], whole, norm_items(1, act_a1, late))
            put(1, products(parity, steps[3:], whole, norm_items(0, act_a0, range(n_blk)), parts))
            weight_copy(layer, parity, 1).wait()
            weight_copy(layer, parity, 0).wait()

            @pl.when(has_prev)
            def _():
                halo_copy(raw.at[1], parity, 1).wait_recv()

            src1 = jnp.where(has_prev, 3 + 2 * parity, 0)
            src0 = jnp.where(has_prev, 2 + 2 * parity, 0)
            parts = products(parity, tap(1, act_a0), whole, norm_items(src1, act_h1, range(n_blk)))
            add(1, products(parity, tap(0, act_h1), whole, [], parts))
            @pl.when(has_next)
            def _():
                halo_copy(raw.at[1], nxt, 1).wait_send()

            @pl.when(layer == 0)
            def _():
                for t in (1, 0):
                    pltpu.make_async_copy(x_hbm.at[t], xres.at[0, t], x_sems.at[2 + t]).wait()

            put(0, products(parity, tap(2, act_a0, (0,)), whole, pops(layer, odd, 1, whole)))
            @pl.when(jnp.logical_and(more, has_next))
            def _():
                halo_copy(raw.at[1], nxt, 1).start()

            @pl.when(jnp.logical_not(more))
            def _():
                pltpu.make_async_copy(raw.at[1], out_hbm.at[1], out_sems.at[1]).start()

            for dist in range(1, n_time):
                stat_copy(parity, dist).wait_send()

            add(0, products(parity, tap(2, act_a0, (-1, 1)), whole, []))
            @pl.when(has_prev)
            def _():
                halo_copy(raw.at[0], parity, 0).wait_recv()

            @pl.when(has_next)
            def _():
                halo_copy(raw.at[0], nxt, 0).wait_send()

            add(0, products(parity, tap(1, act_h1), whole, norm_items(src0, act_h0, range(n_blk))))
            add(0, products(parity, tap(0, act_h0), top, []))
            add(0, products(parity, tap(0, act_h0), low, pops(layer, odd, 0, top)))
            for item in pops(layer, odd, 0, low):
                item()

            @pl.when(more)
            def _():
                send_stats(nxt)

            @pl.when(jnp.logical_not(more))
            def _():
                pltpu.make_async_copy(raw.at[0], out_hbm.at[0], out_sems.at[0]).start()

            return carry

        lax.fori_loop(0, n_layers, layer_step, 0)
        for t in (1, 0):
            pltpu.make_async_copy(raw.at[t], out_hbm.at[t], out_sems.at[t]).wait()

    run_body(accs)


def solution(mesh):
    n_time = mesh.shape["cp"]
    frame_spec = P(("dp", "cp"))

    def local_fn(latent, conv_kernels, conv_biases, gn_gammas, gn_betas):
        n_frames, n_rows, n_cols, n_chans = latent.shape
        n_layers = conv_kernels.shape[0]
        n_taps = conv_kernels.shape[1]
        elem_count = n_time * n_frames * n_rows * n_cols * (n_chans // GROUPS)
        frame = (n_rows * n_cols, n_chans)
        any_spec = pl.BlockSpec(memory_space=pl.ANY)
        decoded = pl.pallas_call(
            functools.partial(_kernel, n_time, n_layers, n_rows, n_cols, n_chans, float(elem_count)),
            out_shape=jax.ShapeDtypeStruct((n_frames,) + frame, BF16),
            in_specs=[any_spec] * 5,
            out_specs=any_spec,
            scratch_shapes=[
                pltpu.VMEM((6,) + frame, BF16),
                pltpu.VMEM((2, n_frames) + frame, BF16),
                pltpu.VMEM((frame[0], 3 * n_chans), BF16),
                pltpu.VMEM((frame[0], 3 * n_chans), BF16),
                pltpu.VMEM((frame[0], 3 * n_chans), BF16),
                pltpu.VMEM((frame[0], 3 * n_chans), BF16),
                pltpu.VMEM((2, n_taps, 9 * n_chans, n_chans), BF16),
                pltpu.VMEM((n_frames,) + frame, F32),
                pltpu.VMEM((2, 8, n_chans), F32),
                pltpu.VMEM((8, n_chans), F32),
                pltpu.VMEM((2, 8, LANES), F32),
                pltpu.VMEM((2, n_time, 8, LANES), F32),
                pltpu.VMEM((3, n_layers, n_chans), F32),
                pltpu.VMEM((n_layers, 1, n_chans), F32),
                pltpu.VMEM((n_layers, 1, n_chans), F32),
                pltpu.VMEM((n_layers, 1, n_chans), F32),
                pltpu.SemaphoreType.DMA((4,)),
                pltpu.SemaphoreType.DMA((3,)),
                pltpu.SemaphoreType.DMA((2, n_taps)),
                pltpu.SemaphoreType.DMA((2,)),
                pltpu.SemaphoreType.DMA((2, 2)),
                pltpu.SemaphoreType.DMA((2, n_time)),
                pltpu.SemaphoreType.DMA((2, n_time)),
                pltpu.SemaphoreType.DMA((2,)),
            ],
            compiler_params=pltpu.CompilerParams(collective_id=0, has_side_effects=True, vmem_limit_bytes=60 * 1024 * 1024),
            name="decoder_blocks",
        )(latent.reshape((n_frames,) + frame), conv_kernels.reshape(n_layers, n_taps, 9 * n_chans, n_chans),
          conv_biases, gn_gammas, gn_betas)
        return decoded.reshape(latent.shape)

    return jax.shard_map(local_fn, mesh=mesh, in_specs=(frame_spec, P(), P(), P(), P()), out_specs=frame_spec, check_vma=False)
```

```python
import functools

import jax
import jax.numpy as jnp
from jax import lax
from jax.experimental import pallas as pl
from jax.experimental.pallas import tpu as pltpu
from jax.sharding import PartitionSpec as P

GROUPS = 32
NORM_EPS = 1e-6
F32 = jnp.float32
BF16 = jnp.bfloat16
MESH = pl.DeviceIdType.MESH
TILE = 256
LANES = 128


def _kernel(n_time, n_layers, n_rows, n_cols, n_chans, elem_count,
            x_hbm, w_hbm, bias_hbm, gamma_hbm, beta_hbm, own,
            halo, xres, act_h0, act_h1, act_a0, act_a1, wbuf, st, ss, stat_tx, stat_rx,
            params_in, bias_ref, gamma_ref, beta_ref, x_sems, p_sems, w_sems, halo_send, halo_recv, stat_send, stat_recv):
    dp = lax.axis_index("dp")
    me = lax.axis_index("cp")
    acts = (act_h0, act_h1, act_a0, act_a1)
    n_blk = n_chans // LANES
    n_half = n_chans // TILE
    frame_rows = n_rows * n_cols
    group_width = n_chans // GROUPS
    has_next = me < n_time - 1
    has_prev = me > 0
    half_rows = n_rows // 2
    n_pieces = 3

    def peer(dist):
        return lax.rem(me + dist, n_time)

    def halo_copies(parity, t):
        pieces = n_pieces if t == 1 else 1
        span = frame_rows // pieces
        return [pltpu.make_async_remote_copy(
            src_ref=own.at[t, i * span:(i + 1) * span], dst_ref=halo.at[2 * parity + t, i * span:(i + 1) * span],
            send_sem=halo_send.at[t, i], recv_sem=halo_recv.at[parity, t, i],
            device_id=(dp, lax.rem(me + 1, n_time)), device_id_type=MESH) for i in range(pieces)]

    def start_halo(cond, parity, t):
        @pl.when(cond)
        def _():
            for copy in halo_copies(parity, t):
                copy.start()

    def sent_halo(parity, t):
        @pl.when(has_next)
        def _():
            for copy in halo_copies(parity, t):
                copy.wait_send()

    def take_halo(parity, t, i):
        @pl.when(has_prev)
        def _():
            halo_copies(parity, t)[i].wait_recv()

    def weight_copy(layer, parity, k):
        return pltpu.make_async_copy(w_hbm.at[layer, k], wbuf.at[parity, k], w_sems.at[parity, k])

    def stat_copy(parity, dist):
        return pltpu.make_async_remote_copy(
            src_ref=stat_tx.at[parity], dst_ref=stat_rx.at[parity, me], send_sem=stat_send.at[parity, dist],
            recv_sem=stat_recv.at[parity], device_id=(dp, peer(dist)), device_id_type=MESH)

    def stat_arrivals(parity):
        return pltpu.make_async_copy(stat_rx.at[parity, 0:n_time - 1], stat_rx.at[parity, 0:n_time - 1], stat_recv.at[parity])

    far_first = sorted(range(1, n_time), key=lambda d: -min(d, n_time - d))

    def send_stats(parity):
        for row in range(2):
            total = jnp.sum(st[row], axis=0, keepdims=True)
            for blk in range(n_blk):
                stat_tx[parity, row * n_blk + blk:row * n_blk + blk + 1, :] = total[:, blk * LANES:(blk + 1) * LANES]
        stat_rx[parity, me] = stat_tx[parity]
        for dist in far_first:
            stat_copy(parity, dist).start()

    def finish_stats(layer, parity):
        stat_arrivals(parity).wait()
        total = stat_rx[parity, 0]
        for src in range(1, n_time):
            total = total + stat_rx[parity, src]
        lane = lax.broadcasted_iota(jnp.int32, total.shape, 1)
        step = 1
        while step < group_width:
            other = jnp.where((lane & step) != 0, pltpu.roll(total, step, 1), pltpu.roll(total, LANES - step, 1))
            total = total + other
            step *= 2
        mean = total[:n_blk] / elem_count
        var = total[n_blk:] / elem_count - mean * mean
        rstd = lax.rsqrt(var + NORM_EPS)
        for blk in range(n_blk):
            lanes = slice(blk * LANES, (blk + 1) * LANES)
            scale = rstd[blk:blk + 1] * gamma_ref[layer, :, lanes]
            ss[0:1, lanes] = scale
            ss[1:2, lanes] = beta_ref[layer, :, lanes] - mean[blk:blk + 1] * scale

    def add_stats(val, lanes):
        grouped = val.reshape(val.shape[0] // 8, 8, val.shape[1])
        st[0, :, lanes] += jnp.sum(grouped, axis=0)
        st[1, :, lanes] += jnp.sum(grouped * grouped, axis=0)

    def norm_item(source, act, row, blk):
        rows = slice(row * n_cols, (row + 1) * n_cols)
        lanes = slice(blk * LANES, (blk + 1) * LANES)
        val = source(rows, lanes)
        val = (val * ss[0:1, lanes] + ss[1:2, lanes]).astype(BF16).astype(F32)
        val = val * lax.logistic(val)
        col = lax.broadcasted_iota(jnp.int32, val.shape, 0)
        act[rows, n_chans + blk * LANES:n_chans + (blk + 1) * LANES] = val.astype(BF16)
        before = jnp.where(col == 0, 0.0, pltpu.roll(val, 1, 0))
        act[rows, blk * LANES:(blk + 1) * LANES] = before.astype(BF16)
        after = jnp.where(col == n_cols - 1, 0.0, pltpu.roll(val, n_cols - 1, 0))
        act[rows, 2 * n_chans + blk * LANES:2 * n_chans + (blk + 1) * LANES] = after.astype(BF16)

    def norm_items(source, act, blks, rows=None):
        return [functools.partial(norm_item, source, act, row, blk) for row in (rows or range(n_rows)) for blk in blks]

    def own_frame(t):
        return lambda rows, lanes: own[t, rows, lanes].astype(F32)

    def halo_frame(parity, t):
        return lambda rows, lanes: jnp.where(has_prev, halo[2 * parity + t, rows, lanes].astype(F32), own[0, rows, lanes].astype(F32))

    def run_body():
        def finish_item(layer, odd, keep, t, row, q, part):
            rows = slice(row * n_cols, (row + 1) * n_cols)
            lanes = slice(q * TILE, (q + 1) * TILE)
            val = part[:, lanes] + bias_ref[layer, :, lanes]
            val = val.astype(BF16).astype(F32)
            old = xres[t, rows, lanes].astype(F32)
            val = (val + old * keep).astype(BF16)
            own[t, rows, lanes] = val
            val = val.astype(F32)
            xres[t, rows, lanes] = jnp.where(odd == 1, val, old).astype(BF16)
            add_stats(val, lanes)

        def products(parity, steps, rows, items, parts=None):
            lo, hi = rows[0], rows[-1] + 1
            done = 0
            parts = dict(parts or {})
            for idx, (k, act, di, chan, width) in enumerate(steps):
                r0, r1 = max(lo, -di), min(hi, n_rows - di)
                rows_in = slice((r0 + di) * n_cols, (r1 + di) * n_cols)
                base = (di + 1) * 3 * n_chans
                prod = None
                if width == n_chans:
                    prod = jnp.dot(act[rows_in, :], wbuf[parity, k, base:base + 3 * n_chans, :], preferred_element_type=F32)
                else:
                    for dj in range(3):
                        at = dj * n_chans + chan
                        term = jnp.dot(act[rows_in, at:at + width], wbuf[parity, k, base + at:base + at + width, :],
                                       preferred_element_type=F32)
                        prod = term if prod is None else prod + term
                for row in range(r0, r1):
                    piece = prod[(row - r0) * n_cols:(row - r0 + 1) * n_cols]
                    parts[row] = piece if row not in parts else parts[row] + piece
                upto = (len(items) * (idx + 1)) // len(steps)
                for item in items[done:upto]:
                    item()
                done = upto
            return parts

        def tap(k, act, row_taps=(0, -1, 1)):
            return [(k, act, di, 0, n_chans) for di in row_taps]

        def tap_halves(k, act):
            return [(k, act, di, chan, n_chans // 2) for chan in (0, n_chans // 2) for di in (0, -1, 1)]

        whole = range(n_rows)
        top = range(half_rows)
        low = range(half_rows, n_rows)

        def finish(layer, odd, keep, t, parts, rows):
            return [functools.partial(finish_item, layer, odd, keep, t, row, q, parts[row]) for row in rows for q in range(n_half)]

        barrier = pltpu.get_barrier_semaphore()
        for dist in range(1, n_time):
            pl.semaphore_signal(barrier, inc=1, device_id=(dp, peer(dist)), device_id_type=MESH)
        for t in (1, 0):
            pltpu.make_async_copy(x_hbm.at[t], own.at[t], x_sems.at[t]).start()
        params = [pltpu.make_async_copy(src, params_in.at[i], p_sems.at[i])
                  for i, src in enumerate((bias_hbm, gamma_hbm, beta_hbm))]
        for copy in params:
            copy.start()
        for k in (2, 1, 0):
            weight_copy(0, 0, k).start()
        for t in (1, 0):
            pltpu.make_async_copy(x_hbm.at[t], xres.at[t], x_sems.at[2 + t]).start()
        st[...] = jnp.zeros_like(st)
        for t in (1, 0):
            pltpu.make_async_copy(x_hbm.at[t], own.at[t], x_sems.at[t]).wait()

            def stat_rows(i, carry, t=t):
                base = pl.multiple_of(i * n_cols, n_cols)
                for q in range(n_half):
                    lanes = slice(q * TILE, (q + 1) * TILE)
                    add_stats(own[t, pl.ds(base, n_cols), lanes].astype(F32), lanes)
                return carry

            lax.fori_loop(0, n_rows, stat_rows, 0)
        pl.semaphore_wait(barrier, n_time - 1)
        send_stats(0)

        start_halo(has_next, 0, 1)

        for i, (copy, dst) in enumerate(zip(params, (bias_ref, gamma_ref, beta_ref))):
            copy.wait()
            for layer in range(n_layers):
                dst[layer] = params_in[i, layer:layer + 1, :]

        def layer_step(layer, carry):
            parity = lax.rem(layer, 2)
            odd = parity
            nxt = 1 - parity
            more = layer < n_layers - 1

            @pl.when(more)
            def _():
                for k in (2, 1, 0):
                    weight_copy(layer + 1, nxt, k).start()

            finish_stats(layer, parity)

            start_halo(jnp.logical_and(has_next, layer > 0), parity, 0)

            st[...] = jnp.zeros_like(st)
            keep = odd.astype(F32)
            early = range(n_blk // 2)
            late = range(n_blk // 2, n_blk)
            for item in norm_items(own_frame(1), act_a1, early):
                item()
            weight_copy(layer, parity, 2).wait()
            steps = tap_halves(2, act_a1)
            frame1 = products(parity, steps[:3], whole, norm_items(own_frame(1), act_a1, late))
            frame1 = products(parity, steps[3:], whole, norm_items(own_frame(0), act_a0, range(n_blk)), frame1)
            weight_copy(layer, parity, 1).wait()
            weight_copy(layer, parity, 0).wait()

            take_halo(parity, 1, 0)
            sent_halo(nxt, 1)
            start_halo(jnp.logical_and(has_next, layer == 0), parity, 0)

            @pl.when(layer == 0)
            def _():
                for t in (1, 0):
                    pltpu.make_async_copy(x_hbm.at[t], xres.at[t], x_sems.at[2 + t]).wait()

            for i, di in enumerate((0, -1, 1)):
                if i > 0:
                    take_halo(parity, 1, i)
                items = norm_items(halo_frame(parity, 1), act_h1, range(n_blk), range(2 * i, 2 * i + 2))
                frame1 = products(parity, tap(1, act_a0, (di,)), whole, items, frame1)
            frame1 = products(parity, tap(0, act_h1), top, [], frame1)
            frame1 = products(parity, tap(0, act_h1), low, finish(layer, odd, keep, 1, frame1, top), frame1)
            frame0 = products(parity, tap(2, act_a0, (0,)), whole, finish(layer, odd, keep, 1, frame1, low))
            start_halo(jnp.logical_and(more, has_next), nxt, 1)

            for dist in range(1, n_time):
                stat_copy(parity, dist).wait_send()

            frame0 = products(parity, tap(2, act_a0, (-1, 1)), whole, [], frame0)
            take_halo(parity, 0, 0)
            sent_halo(nxt, 0)

            frame0 = products(parity, tap(1, act_h1), whole, norm_items(halo_frame(parity, 0), act_h0, range(n_blk)), frame0)
            frame0 = products(parity, tap(0, act_h0), top, [], frame0)
            frame0 = products(parity, tap(0, act_h0), low, finish(layer, odd, keep, 0, frame0, top), frame0)
            for item in finish(layer, odd, keep, 0, frame0, low):
                item()

            @pl.when(more)
            def _():
                send_stats(nxt)

            return carry

        lax.fori_loop(0, n_layers, layer_step, 0)

    run_body()


def solution(mesh):
    n_time = mesh.shape["cp"]
    frame_spec = P(("dp", "cp"))

    def local_fn(latent, conv_kernels, conv_biases, gn_gammas, gn_betas):
        n_frames, n_rows, n_cols, n_chans = latent.shape
        n_layers = conv_kernels.shape[0]
        n_taps = conv_kernels.shape[1]
        elem_count = n_time * n_frames * n_rows * n_cols * (n_chans // GROUPS)
        frame = (n_rows * n_cols, n_chans)
        any_spec = pl.BlockSpec(memory_space=pl.ANY)
        decoded = pl.pallas_call(
            functools.partial(_kernel, n_time, n_layers, n_rows, n_cols, n_chans, float(elem_count)),
            out_shape=pltpu.VMEM((n_frames,) + frame, BF16),
            in_specs=[any_spec] * 5,
            out_specs=pl.BlockSpec(memory_space=pltpu.VMEM),
            scratch_shapes=[
                pltpu.VMEM((4,) + frame, BF16),
                pltpu.VMEM((n_frames,) + frame, BF16),
                pltpu.VMEM((frame[0], 3 * n_chans), BF16),
                pltpu.VMEM((frame[0], 3 * n_chans), BF16),
                pltpu.VMEM((frame[0], 3 * n_chans), BF16),
                pltpu.VMEM((frame[0], 3 * n_chans), BF16),
                pltpu.VMEM((2, n_taps, 9 * n_chans, n_chans), BF16),
                pltpu.VMEM((2, 8, n_chans), F32),
                pltpu.VMEM((8, n_chans), F32),
                pltpu.VMEM((2, 8, LANES), F32),
                pltpu.VMEM((2, n_time, 8, LANES), F32),
                pltpu.VMEM((3, n_layers, n_chans), F32),
                pltpu.VMEM((n_layers, 1, n_chans), F32),
                pltpu.VMEM((n_layers, 1, n_chans), F32),
                pltpu.VMEM((n_layers, 1, n_chans), F32),
                pltpu.SemaphoreType.DMA((4,)),
                pltpu.SemaphoreType.DMA((3,)),
                pltpu.SemaphoreType.DMA((2, n_taps)),
                pltpu.SemaphoreType.DMA((2, 3)),
                pltpu.SemaphoreType.DMA((2, 2, 3)),
                pltpu.SemaphoreType.DMA((2, n_time)),
                pltpu.SemaphoreType.DMA((2,)),
            ],
            compiler_params=pltpu.CompilerParams(collective_id=0, has_side_effects=True, vmem_limit_bytes=60 * 1024 * 1024),
            name="decoder_blocks",
        )(latent.reshape((n_frames,) + frame), conv_kernels.reshape(n_layers, n_taps, 9 * n_chans, n_chans),
          conv_biases, gn_gammas, gn_betas)
        return decoded.reshape(latent.shape)

    return jax.shard_map(local_fn, mesh=mesh, in_specs=(frame_spec, P(), P(), P(), P()), out_specs=frame_spec, check_vma=False)
```

```python
import functools

import jax
import jax.numpy as jnp
from jax import lax
from jax.experimental import pallas as pl
from jax.experimental.pallas import tpu as pltpu
from jax.sharding import PartitionSpec as P

GROUPS = 32
NORM_EPS = 1e-6
F32 = jnp.float32
BF16 = jnp.bfloat16
MESH = pl.DeviceIdType.MESH
TILE = 256
LANES = 128


def _kernel(n_time, n_layers, n_rows, n_cols, n_chans, elem_count,
            x_hbm, w_hbm, bias_hbm, gamma_hbm, beta_hbm, own,
            halo, xres, act_h0, act_h1, act_a0, act_a1, wbuf, st, ss, stat_tx, stat_rx,
            params_in, bias_ref, gamma_ref, beta_ref, x_sems, p_sems, w_sems, halo_send, halo_recv, stat_send, stat_recv):
    dp = lax.axis_index("dp")
    me = lax.axis_index("cp")
    acts = (act_h0, act_h1, act_a0, act_a1)
    n_blk = n_chans // LANES
    n_half = n_chans // TILE
    frame_rows = n_rows * n_cols
    group_width = n_chans // GROUPS
    has_next = me < n_time - 1
    has_prev = me > 0
    half_rows = n_rows // 2
    n_pieces = 3

    def peer(dist):
        return lax.rem(me + dist, n_time)

    def halo_copies(parity, t):
        pieces = n_pieces if t == 1 else 1
        span = frame_rows // pieces
        return [pltpu.make_async_remote_copy(
            src_ref=own.at[t, i * span:(i + 1) * span], dst_ref=halo.at[2 * parity + t, i * span:(i + 1) * span],
            send_sem=halo_send.at[t, i], recv_sem=halo_recv.at[parity, t, i],
            device_id=(dp, lax.rem(me + 1, n_time)), device_id_type=MESH) for i in range(pieces)]

    def start_halo(cond, parity, t):
        @pl.when(cond)
        def _():
            for copy in halo_copies(parity, t):
                copy.start()

    def sent_halo(parity, t):
        @pl.when(has_next)
        def _():
            for copy in halo_copies(parity, t):
                copy.wait_send()

    def take_halo(parity, t, i):
        @pl.when(has_prev)
        def _():
            halo_copies(parity, t)[i].wait_recv()

    def weight_copy(layer, parity, k):
        return pltpu.make_async_copy(w_hbm.at[layer, k], wbuf.at[parity, k], w_sems.at[parity, k])

    def stat_copy(parity, dist):
        return pltpu.make_async_remote_copy(
            src_ref=stat_tx.at[parity], dst_ref=stat_rx.at[parity, me], send_sem=stat_send.at[parity, dist],
            recv_sem=stat_recv.at[parity], device_id=(dp, peer(dist)), device_id_type=MESH)

    def tree_sum(terms):
        while len(terms) > 1:
            terms = [terms[i] + terms[i + 1] if i + 1 < len(terms) else terms[i] for i in range(0, len(terms), 2)]
        return terms[0]

    def stat_arrivals(parity):
        return pltpu.make_async_copy(stat_rx.at[parity, 0:n_time - 1], stat_rx.at[parity, 0:n_time - 1], stat_recv.at[parity])

    far_first = sorted(range(1, n_time), key=lambda d: -min(d, n_time - d))

    def send_stats(parity):
        for row in range(2):
            total = jnp.sum(st[row], axis=0, keepdims=True)
            for blk in range(n_blk):
                stat_tx[parity, row * n_blk + blk:row * n_blk + blk + 1, :] = total[:, blk * LANES:(blk + 1) * LANES]
        stat_rx[parity, me] = stat_tx[parity]
        for dist in far_first:
            stat_copy(parity, dist).start()

    def finish_stats(layer, parity):
        stat_arrivals(parity).wait()
        total = tree_sum([stat_rx[parity, src] for src in range(n_time)])
        lane = lax.broadcasted_iota(jnp.int32, total.shape, 1)
        place = lane & (group_width - 1)
        terms = [total]
        for shift in range(1, group_width):
            terms.append(jnp.where(place >= shift, pltpu.roll(total, shift, 1), 0.0))
            terms.append(jnp.where(place < group_width - shift, pltpu.roll(total, LANES - shift, 1), 0.0))
        total = tree_sum(terms)
        mean = total[:n_blk] / elem_count
        var = total[n_blk:] / elem_count - mean * mean
        rstd = lax.rsqrt(var + NORM_EPS)
        for blk in range(n_blk):
            lanes = slice(blk * LANES, (blk + 1) * LANES)
            scale = rstd[blk:blk + 1] * gamma_ref[layer, :, lanes]
            ss[0:1, lanes] = scale
            ss[1:2, lanes] = beta_ref[layer, :, lanes] - mean[blk:blk + 1] * scale

    def add_stats(val, lanes):
        grouped = val.reshape(val.shape[0] // 8, 8, val.shape[1])
        st[0, :, lanes] += jnp.sum(grouped, axis=0)
        st[1, :, lanes] += jnp.sum(grouped * grouped, axis=0)

    def norm_item(source, act, row, blk):
        rows = slice(row * n_cols, (row + 1) * n_cols)
        lanes = slice(blk * LANES, (blk + 1) * LANES)
        val = source(rows, lanes)
        val = (val * ss[0:1, lanes] + ss[1:2, lanes]).astype(BF16).astype(F32)
        val = val * lax.logistic(val)
        col = lax.broadcasted_iota(jnp.int32, (8, LANES), 0)
        act[rows, n_chans + blk * LANES:n_chans + (blk + 1) * LANES] = val.astype(BF16)
        before = pltpu.roll(val, 1, 0)
        before = jnp.concatenate([jnp.where(col == 0, 0.0, before[:8]), before[8:]], axis=0)
        act[rows, blk * LANES:(blk + 1) * LANES] = before.astype(BF16)
        after = pltpu.roll(val, n_cols - 1, 0)
        after = jnp.concatenate([after[:-8], jnp.where(col == 7, 0.0, after[-8:])], axis=0)
        act[rows, 2 * n_chans + blk * LANES:2 * n_chans + (blk + 1) * LANES] = after.astype(BF16)

    def norm_items(source, act, blks, rows=None):
        return [functools.partial(norm_item, source, act, row, blk) for row in (rows or range(n_rows)) for blk in blks]

    def own_frame(t):
        return lambda rows, lanes: own[t, rows, lanes].astype(F32)

    def halo_frame(parity, t):
        return lambda rows, lanes: jnp.where(has_prev, halo[2 * parity + t, rows, lanes].astype(F32), own[0, rows, lanes].astype(F32))

    def run_body():
        def finish_item(layer, odd, t, row, q, part):
            rows = slice(row * n_cols, (row + 1) * n_cols)
            lanes = slice(q * TILE, (q + 1) * TILE)
            val = part[:, lanes] + bias_ref[layer, :, lanes]
            val = val.astype(BF16)
            if odd:
                val = (val.astype(F32) + xres[t, rows, lanes].astype(F32)).astype(BF16)
                xres[t, rows, lanes] = val
            own[t, rows, lanes] = val
            add_stats(val.astype(F32), lanes)

        def products(parity, steps, rows, items, parts=None):
            lo, hi = rows[0], rows[-1] + 1
            done = 0
            parts = dict(parts or {})
            for idx, (k, act, di, chan, width) in enumerate(steps):
                r0, r1 = max(lo, -di), min(hi, n_rows - di)
                rows_in = slice((r0 + di) * n_cols, (r1 + di) * n_cols)
                base = (di + 1) * 3 * n_chans
                prod = None
                if width == n_chans:
                    prod = jnp.dot(act[rows_in, :], wbuf[parity, k, base:base + 3 * n_chans, :], preferred_element_type=F32)
                else:
                    for dj in range(3):
                        at = dj * n_chans + chan
                        term = jnp.dot(act[rows_in, at:at + width], wbuf[parity, k, base + at:base + at + width, :],
                                       preferred_element_type=F32)
                        prod = term if prod is None else prod + term
                for row in range(r0, r1):
                    piece = prod[(row - r0) * n_cols:(row - r0 + 1) * n_cols]
                    parts[row] = piece if row not in parts else parts[row] + piece
                upto = (len(items) * (idx + 1)) // len(steps)
                for item in items[done:upto]:
                    item()
                done = upto
            return parts

        def tap(k, act, row_taps=(0, -1, 1)):
            return [(k, act, di, 0, n_chans) for di in row_taps]

        def tap_halves(k, act):
            return [(k, act, di, chan, n_chans // 2) for chan in (0, n_chans // 2) for di in (0, -1, 1)]

        whole = range(n_rows)
        top = range(half_rows)
        low = range(half_rows, n_rows)

        def finish(layer, odd, t, parts, rows):
            return [functools.partial(finish_item, layer, odd, t, row, q, parts[row]) for row in rows for q in range(n_half)]

        barrier = pltpu.get_barrier_semaphore()
        for dist in far_first:
            pl.semaphore_signal(barrier, inc=1, device_id=(dp, peer(dist)), device_id_type=MESH)
        for t in (1, 0):
            pltpu.make_async_copy(x_hbm.at[t], own.at[t], x_sems.at[t]).start()
        params = [pltpu.make_async_copy(src, params_in.at[i], p_sems.at[i])
                  for i, src in enumerate((bias_hbm, gamma_hbm, beta_hbm))]
        for copy in params:
            copy.start()
        for k in (2, 1, 0):
            weight_copy(0, 0, k).start()
        for t in (1, 0):
            pltpu.make_async_copy(x_hbm.at[t], xres.at[t], x_sems.at[2 + t]).start()
        st[...] = jnp.zeros_like(st)
        for t in (1, 0):
            pltpu.make_async_copy(x_hbm.at[t], own.at[t], x_sems.at[t]).wait()

            def stat_rows(i, carry, t=t):
                base = pl.multiple_of(i * n_cols, n_cols)
                for q in range(n_half):
                    lanes = slice(q * TILE, (q + 1) * TILE)
                    add_stats(own[t, pl.ds(base, n_cols), lanes].astype(F32), lanes)
                return carry

            lax.fori_loop(0, n_rows, stat_rows, 0)
        pl.semaphore_wait(barrier, n_time - 1)
        send_stats(0)

        start_halo(has_next, 0, 1)

        for i, (copy, dst) in enumerate(zip(params, (bias_ref, gamma_ref, beta_ref))):
            copy.wait()
            for layer in range(n_layers):
                dst[layer] = params_in[i, layer:layer + 1, :]

        def layer_step(layer, parity):
            odd = parity == 1
            nxt = 1 - parity
            more = layer < n_layers - 1

            @pl.when(more)
            def _():
                for k in (2, 1, 0):
                    weight_copy(layer + 1, nxt, k).start()

            finish_stats(layer, parity)

            start_halo(jnp.logical_and(has_next, layer > 0), parity, 0)

            st[...] = jnp.zeros_like(st)
            early = range(n_blk // 2)
            late = range(n_blk // 2, n_blk)
            for item in norm_items(own_frame(1), act_a1, early):
                item()
            weight_copy(layer, parity, 2).wait()
            steps = tap_halves(2, act_a1)
            frame1 = products(parity, steps[:3], whole, norm_items(own_frame(1), act_a1, late))
            frame1 = products(parity, steps[3:], whole, norm_items(own_frame(0), act_a0, range(n_blk)), frame1)
            weight_copy(layer, parity, 1).wait()
            weight_copy(layer, parity, 0).wait()

            take_halo(parity, 1, 0)
            start_halo(jnp.logical_and(has_next, layer == 0), parity, 0)

            @pl.when(layer == 0)
            def _():
                for t in (1, 0):
                    pltpu.make_async_copy(x_hbm.at[t], xres.at[t], x_sems.at[2 + t]).wait()

            for i, di in enumerate((0, -1, 1)):
                if i > 0:
                    take_halo(parity, 1, i)
                items = norm_items(halo_frame(parity, 1), act_h1, range(n_blk), range(2 * i, 2 * i + 2))
                frame1 = products(parity, tap(1, act_a0, (di,)), whole, items, frame1)
            frame1 = products(parity, tap(0, act_h1), top, [], frame1)
            sent_halo(nxt, 1)
            frame1 = products(parity, tap(0, act_h1), low, finish(layer, odd, 1, frame1, top), frame1)
            frame0 = products(parity, tap(2, act_a0, (0,)), whole, finish(layer, odd, 1, frame1, low))
            start_halo(jnp.logical_and(more, has_next), nxt, 1)

            for dist in range(1, n_time):
                stat_copy(parity, dist).wait_send()

            frame0 = products(parity, tap(2, act_a0, (-1, 1)), whole, [], frame0)
            take_halo(parity, 0, 0)
            sent_halo(nxt, 0)

            frame0 = products(parity, tap(1, act_h1), whole, norm_items(halo_frame(parity, 0), act_h0, range(n_blk)), frame0)
            frame0 = products(parity, tap(0, act_h0), top, [], frame0)
            frame0 = products(parity, tap(0, act_h0), low, finish(layer, odd, 0, frame0, top), frame0)
            for item in finish(layer, odd, 0, frame0, low):
                item()

            @pl.when(more)
            def _():
                send_stats(nxt)

        def block_step(block, carry):
            for parity in range(2):
                layer_step(2 * block + parity, parity)
            return carry

        lax.fori_loop(0, n_layers // 2, block_step, 0)

    run_body()


def solution(mesh):
    n_time = mesh.shape["cp"]
    frame_spec = P(("dp", "cp"))

    def local_fn(latent, conv_kernels, conv_biases, gn_gammas, gn_betas):
        n_frames, n_rows, n_cols, n_chans = latent.shape
        n_layers = conv_kernels.shape[0]
        n_taps = conv_kernels.shape[1]
        elem_count = n_time * n_frames * n_rows * n_cols * (n_chans // GROUPS)
        frame = (n_rows * n_cols, n_chans)
        any_spec = pl.BlockSpec(memory_space=pl.ANY)
        decoded = pl.pallas_call(
            functools.partial(_kernel, n_time, n_layers, n_rows, n_cols, n_chans, float(elem_count)),
            out_shape=pltpu.VMEM((n_frames,) + frame, BF16),
            in_specs=[any_spec] * 5,
            out_specs=pl.BlockSpec(memory_space=pltpu.VMEM),
            scratch_shapes=[
                pltpu.VMEM((4,) + frame, BF16),
                pltpu.VMEM((n_frames,) + frame, BF16),
                pltpu.VMEM((frame[0], 3 * n_chans), BF16),
                pltpu.VMEM((frame[0], 3 * n_chans), BF16),
                pltpu.VMEM((frame[0], 3 * n_chans), BF16),
                pltpu.VMEM((frame[0], 3 * n_chans), BF16),
                pltpu.VMEM((2, n_taps, 9 * n_chans, n_chans), BF16),
                pltpu.VMEM((2, 8, n_chans), F32),
                pltpu.VMEM((8, n_chans), F32),
                pltpu.VMEM((2, 8, LANES), F32),
                pltpu.VMEM((2, n_time, 8, LANES), F32),
                pltpu.VMEM((3, n_layers, n_chans), F32),
                pltpu.VMEM((n_layers, 1, n_chans), F32),
                pltpu.VMEM((n_layers, 1, n_chans), F32),
                pltpu.VMEM((n_layers, 1, n_chans), F32),
                pltpu.SemaphoreType.DMA((4,)),
                pltpu.SemaphoreType.DMA((3,)),
                pltpu.SemaphoreType.DMA((2, n_taps)),
                pltpu.SemaphoreType.DMA((2, 3)),
                pltpu.SemaphoreType.DMA((2, 2, 3)),
                pltpu.SemaphoreType.DMA((2, n_time)),
                pltpu.SemaphoreType.DMA((2,)),
            ],
            compiler_params=pltpu.CompilerParams(collective_id=0, has_side_effects=True, vmem_limit_bytes=60 * 1024 * 1024),
            name="decoder_blocks",
        )(latent.reshape((n_frames,) + frame), conv_kernels.reshape(n_layers, n_taps, 9 * n_chans, n_chans),
          conv_biases, gn_gammas, gn_betas)
        return decoded.reshape(latent.shape)

    return jax.shard_map(local_fn, mesh=mesh, in_specs=(frame_spec, P(), P(), P(), P()), out_specs=frame_spec, check_vma=False)
```

```python
import functools

import jax
import jax.numpy as jnp
from jax import lax
from jax.experimental import pallas as pl
from jax.experimental.pallas import tpu as pltpu
from jax.sharding import PartitionSpec as P

GROUPS = 32
NORM_EPS = 1e-6
F32 = jnp.float32
BF16 = jnp.bfloat16
MESH = pl.DeviceIdType.MESH
TILE = 256
LANES = 128


def _kernel(n_time, n_layers, n_rows, n_cols, n_chans, elem_count,
            x_hbm, w_hbm, bias_hbm, gamma_hbm, beta_hbm, own,
            halo, xres, act_h0, act_h1, act_a0, act_a1, wbuf, st, ss, stat_tx, stat_rx,
            params_in, bias_ref, gamma_ref, beta_ref, x_sems, p_sems, w_sems, halo_send, halo_recv, stat_send, stat_recv):
    dp = lax.axis_index("dp")
    me = lax.axis_index("cp")
    acts = (act_h0, act_h1, act_a0, act_a1)
    n_blk = n_chans // LANES
    n_half = n_chans // TILE
    frame_rows = n_rows * n_cols
    group_width = n_chans // GROUPS
    has_next = me < n_time - 1
    has_prev = me > 0
    half_rows = n_rows // 2
    n_pieces = 3

    def peer(dist):
        return lax.rem(me + dist, n_time)

    def halo_copies(parity, t):
        pieces = n_pieces if t == 1 else 1
        span = frame_rows // pieces
        return [pltpu.make_async_remote_copy(
            src_ref=own.at[t, i * span:(i + 1) * span], dst_ref=halo.at[2 * parity + t, i * span:(i + 1) * span],
            send_sem=halo_send.at[t, i], recv_sem=halo_recv.at[parity, t, i],
            device_id=(dp, lax.rem(me + 1, n_time)), device_id_type=MESH) for i in range(pieces)]

    def start_halo(cond, parity, t):
        @pl.when(cond)
        def _():
            for copy in halo_copies(parity, t):
                copy.start()

    def sent_halo(parity, t):
        @pl.when(has_next)
        def _():
            for copy in halo_copies(parity, t):
                copy.wait_send()

    def take_halo(parity, t, i):
        @pl.when(has_prev)
        def _():
            halo_copies(parity, t)[i].wait_recv()

    def weight_copy(layer, parity, k):
        return pltpu.make_async_copy(w_hbm.at[layer, k], wbuf.at[parity, k], w_sems.at[parity, k])

    def stat_copy(parity, dist):
        return pltpu.make_async_remote_copy(
            src_ref=stat_tx.at[parity], dst_ref=stat_rx.at[parity, me], send_sem=stat_send.at[parity, dist],
            recv_sem=stat_recv.at[parity], device_id=(dp, peer(dist)), device_id_type=MESH)

    def tree_sum(terms):
        while len(terms) > 1:
            terms = [terms[i] + terms[i + 1] if i + 1 < len(terms) else terms[i] for i in range(0, len(terms), 2)]
        return terms[0]

    def stat_arrivals(parity):
        return pltpu.make_async_copy(stat_rx.at[parity, 0:n_time - 1], stat_rx.at[parity, 0:n_time - 1], stat_recv.at[parity])

    far_first = sorted(range(1, n_time), key=lambda d: -min(d, n_time - d))

    def send_stats(parity):
        for row in range(2):
            total = jnp.sum(st[row], axis=0, keepdims=True)
            for blk in range(n_blk):
                stat_tx[parity, row * n_blk + blk:row * n_blk + blk + 1, :] = total[:, blk * LANES:(blk + 1) * LANES]
        stat_rx[parity, me] = stat_tx[parity]
        for dist in far_first:
            stat_copy(parity, dist).start()

    def finish_stats(layer, parity):
        stat_arrivals(parity).wait()
        total = tree_sum([stat_rx[parity, src] for src in range(n_time)])
        lane = lax.broadcasted_iota(jnp.int32, total.shape, 1)
        place = lane & (group_width - 1)
        terms = [total]
        for shift in range(1, group_width):
            terms.append(jnp.where(place >= shift, pltpu.roll(total, shift, 1), 0.0))
            terms.append(jnp.where(place < group_width - shift, pltpu.roll(total, LANES - shift, 1), 0.0))
        total = tree_sum(terms)
        mean = total[:n_blk] / elem_count
        var = total[n_blk:] / elem_count - mean * mean
        rstd = lax.rsqrt(var + NORM_EPS)
        for blk in range(n_blk):
            lanes = slice(blk * LANES, (blk + 1) * LANES)
            scale = rstd[blk:blk + 1] * gamma_ref[layer, :, lanes]
            ss[0:1, lanes] = scale
            ss[1:2, lanes] = beta_ref[layer, :, lanes] - mean[blk:blk + 1] * scale

    def add_stats(val, lanes):
        grouped = val.reshape(val.shape[0] // 8, 8, val.shape[1])
        st[0, :, lanes] += jnp.sum(grouped, axis=0)
        st[1, :, lanes] += jnp.sum(grouped * grouped, axis=0)

    def norm_item(source, act, row, blk):
        rows = slice(row * n_cols, (row + 1) * n_cols)
        lanes = slice(blk * LANES, (blk + 1) * LANES)
        val = source(rows, lanes)
        val = (val * ss[0:1, lanes] + ss[1:2, lanes]).astype(BF16).astype(F32)
        val = val * lax.logistic(val)
        col = lax.broadcasted_iota(jnp.int32, (8, LANES), 0)
        act[rows, n_chans + blk * LANES:n_chans + (blk + 1) * LANES] = val.astype(BF16)
        before = pltpu.roll(val, 1, 0)
        before = jnp.concatenate([jnp.where(col == 0, 0.0, before[:8]), before[8:]], axis=0)
        act[rows, blk * LANES:(blk + 1) * LANES] = before.astype(BF16)
        after = pltpu.roll(val, n_cols - 1, 0)
        after = jnp.concatenate([after[:-8], jnp.where(col == 7, 0.0, after[-8:])], axis=0)
        act[rows, 2 * n_chans + blk * LANES:2 * n_chans + (blk + 1) * LANES] = after.astype(BF16)

    def norm_items(source, act, blks, rows=None):
        return [functools.partial(norm_item, source, act, row, blk) for row in (rows or range(n_rows)) for blk in blks]

    def own_frame(t):
        return lambda rows, lanes: own[t, rows, lanes].astype(F32)

    def halo_frame(parity, t):
        return lambda rows, lanes: jnp.where(has_prev, halo[2 * parity + t, rows, lanes].astype(F32), own[0, rows, lanes].astype(F32))

    def run_body():
        def finish_item(layer, odd, t, row, q, part):
            rows = slice(row * n_cols, (row + 1) * n_cols)
            lanes = slice(q * TILE, (q + 1) * TILE)
            val = part[:, lanes] + bias_ref[layer, :, lanes]
            val = val.astype(BF16)
            if odd:
                val = (val.astype(F32) + xres[t, rows, lanes].astype(F32)).astype(BF16)
                xres[t, rows, lanes] = val
            own[t, rows, lanes] = val
            add_stats(val.astype(F32), lanes)

        def products(parity, steps, rows, items, parts=None):
            lo, hi = rows[0], rows[-1] + 1
            done = 0
            parts = dict(parts or {})
            for idx, (k, act, di, chan, width) in enumerate(steps):
                r0, r1 = max(lo, -di), min(hi, n_rows - di)
                rows_in = slice((r0 + di) * n_cols, (r1 + di) * n_cols)
                base = (di + 1) * 3 * n_chans
                prod = None
                if width == n_chans:
                    prod = jnp.dot(act[rows_in, :], wbuf[parity, k, base:base + 3 * n_chans, :], preferred_element_type=F32)
                else:
                    for dj in range(3):
                        at = dj * n_chans + chan
                        term = jnp.dot(act[rows_in, at:at + width], wbuf[parity, k, base + at:base + at + width, :],
                                       preferred_element_type=F32)
                        prod = term if prod is None else prod + term
                for row in range(r0, r1):
                    piece = prod[(row - r0) * n_cols:(row - r0 + 1) * n_cols]
                    parts[row] = piece if row not in parts else parts[row] + piece
                upto = (len(items) * (idx + 1)) // len(steps)
                for item in items[done:upto]:
                    item()
                done = upto
            return parts

        def tap(k, act, row_taps=(0, -1, 1)):
            return [(k, act, di, 0, n_chans) for di in row_taps]

        def tap_halves(k, act):
            return [(k, act, di, chan, n_chans // 2) for chan in (0, n_chans // 2) for di in (0, -1, 1)]

        whole = range(n_rows)
        top = range(half_rows)
        low = range(half_rows, n_rows)

        def finish(layer, odd, t, parts, rows):
            return [functools.partial(finish_item, layer, odd, t, row, q, parts[row]) for row in rows for q in range(n_half)]

        barrier = pltpu.get_barrier_semaphore()
        for dist in far_first:
            pl.semaphore_signal(barrier, inc=1, device_id=(dp, peer(dist)), device_id_type=MESH)
        for t in (1, 0):
            pltpu.make_async_copy(x_hbm.at[t], own.at[t], x_sems.at[t]).start()
        params = [pltpu.make_async_copy(src, params_in.at[i], p_sems.at[i])
                  for i, src in enumerate((bias_hbm, gamma_hbm, beta_hbm))]
        for copy in params:
            copy.start()
        for k in (2, 1, 0):
            weight_copy(0, 0, k).start()
        for t in (1, 0):
            pltpu.make_async_copy(x_hbm.at[t], xres.at[t], x_sems.at[2 + t]).start()
        st[...] = jnp.zeros_like(st)
        for t in (1, 0):
            pltpu.make_async_copy(x_hbm.at[t], own.at[t], x_sems.at[t]).wait()

            def stat_rows(i, carry, t=t):
                base = pl.multiple_of(i * n_cols, n_cols)
                for q in range(n_half):
                    lanes = slice(q * TILE, (q + 1) * TILE)
                    add_stats(own[t, pl.ds(base, n_cols), lanes].astype(F32), lanes)
                return carry

            lax.fori_loop(0, n_rows, stat_rows, 0)
        pl.semaphore_wait(barrier, n_time - 1)
        send_stats(0)

        start_halo(has_next, 0, 1)

        for i, (copy, dst) in enumerate(zip(params, (bias_ref, gamma_ref, beta_ref))):
            copy.wait()
            for layer in range(n_layers):
                dst[layer] = params_in[i, layer:layer + 1, :]

        def layer_step(layer, parity):
            odd = parity == 1
            nxt = 1 - parity
            more = layer < n_layers - 1

            @pl.when(more)
            def _():
                for k in (2, 1, 0):
                    weight_copy(layer + 1, nxt, k).start()

            finish_stats(layer, parity)
            for dist in range(1, n_time):
                stat_copy(parity, dist).wait_send()

            start_halo(jnp.logical_and(has_next, layer > 0), parity, 0)

            st[...] = jnp.zeros_like(st)
            early = range(n_blk // 2)
            late = range(n_blk // 2, n_blk)
            for item in norm_items(own_frame(1), act_a1, early):
                item()
            weight_copy(layer, parity, 2).wait()
            steps = tap_halves(2, act_a1)
            frame1 = products(parity, steps[:3], whole, norm_items(own_frame(1), act_a1, late))
            frame1 = products(parity, steps[3:], whole, norm_items(own_frame(0), act_a0, range(n_blk)), frame1)
            weight_copy(layer, parity, 1).wait()
            weight_copy(layer, parity, 0).wait()

            take_halo(parity, 1, 0)
            start_halo(jnp.logical_and(has_next, layer == 0), parity, 0)

            @pl.when(layer == 0)
            def _():
                for t in (1, 0):
                    pltpu.make_async_copy(x_hbm.at[t], xres.at[t], x_sems.at[2 + t]).wait()

            for i, di in enumerate((0, -1, 1)):
                if i > 0:
                    take_halo(parity, 1, i)
                items = norm_items(halo_frame(parity, 1), act_h1, range(n_blk), range(2 * i, 2 * i + 2))
                frame1 = products(parity, tap(1, act_a0, (di,)), whole, items, frame1)
            frame1 = products(parity, tap(0, act_h1), whole, [], frame1)
            sent_halo(nxt, 1)
            frame0 = products(parity, tap(2, act_a0, (0,)), whole, finish(layer, odd, 1, frame1, whole))
            start_halo(jnp.logical_and(more, has_next), nxt, 1)

            frame0 = products(parity, tap(2, act_a0, (-1, 1)), whole, [], frame0)
            take_halo(parity, 0, 0)
            sent_halo(nxt, 0)

            frame0 = products(parity, tap(1, act_h1), whole, norm_items(halo_frame(parity, 0), act_h0, range(n_blk)), frame0)
            frame0 = products(parity, tap(0, act_h0), top, [], frame0)
            frame0 = products(parity, tap(0, act_h0), low, finish(layer, odd, 0, frame0, top), frame0)
            for item in finish(layer, odd, 0, frame0, low):
                item()

            @pl.when(more)
            def _():
                send_stats(nxt)

        def block_step(block, carry):
            for parity in range(2):
                layer_step(2 * block + parity, parity)
            return carry

        lax.fori_loop(0, n_layers // 2, block_step, 0)

    run_body()


def solution(mesh):
    n_time = mesh.shape["cp"]
    frame_spec = P(("dp", "cp"))

    def local_fn(latent, conv_kernels, conv_biases, gn_gammas, gn_betas):
        n_frames, n_rows, n_cols, n_chans = latent.shape
        n_layers = conv_kernels.shape[0]
        n_taps = conv_kernels.shape[1]
        elem_count = n_time * n_frames * n_rows * n_cols * (n_chans // GROUPS)
        frame = (n_rows * n_cols, n_chans)
        any_spec = pl.BlockSpec(memory_space=pl.ANY)
        decoded = pl.pallas_call(
            functools.partial(_kernel, n_time, n_layers, n_rows, n_cols, n_chans, float(elem_count)),
            out_shape=pltpu.VMEM((n_frames,) + frame, BF16),
            in_specs=[any_spec] * 5,
            out_specs=pl.BlockSpec(memory_space=pltpu.VMEM),
            scratch_shapes=[
                pltpu.VMEM((4,) + frame, BF16),
                pltpu.VMEM((n_frames,) + frame, BF16),
                pltpu.VMEM((frame[0], 3 * n_chans), BF16),
                pltpu.VMEM((frame[0], 3 * n_chans), BF16),
                pltpu.VMEM((frame[0], 3 * n_chans), BF16),
                pltpu.VMEM((frame[0], 3 * n_chans), BF16),
                pltpu.VMEM((2, n_taps, 9 * n_chans, n_chans), BF16),
                pltpu.VMEM((2, 8, n_chans), F32),
                pltpu.VMEM((8, n_chans), F32),
                pltpu.VMEM((2, 8, LANES), F32),
                pltpu.VMEM((2, n_time, 8, LANES), F32),
                pltpu.VMEM((3, n_layers, n_chans), F32),
                pltpu.VMEM((n_layers, 1, n_chans), F32),
                pltpu.VMEM((n_layers, 1, n_chans), F32),
                pltpu.VMEM((n_layers, 1, n_chans), F32),
                pltpu.SemaphoreType.DMA((4,)),
                pltpu.SemaphoreType.DMA((3,)),
                pltpu.SemaphoreType.DMA((2, n_taps)),
                pltpu.SemaphoreType.DMA((2, 3)),
                pltpu.SemaphoreType.DMA((2, 2, 3)),
                pltpu.SemaphoreType.DMA((2, n_time)),
                pltpu.SemaphoreType.DMA((2,)),
            ],
            compiler_params=pltpu.CompilerParams(collective_id=0, has_side_effects=True, vmem_limit_bytes=60 * 1024 * 1024),
            name="decoder_blocks",
        )(latent.reshape((n_frames,) + frame), conv_kernels.reshape(n_layers, n_taps, 9 * n_chans, n_chans),
          conv_biases, gn_gammas, gn_betas)
        return decoded.reshape(latent.shape)

    return jax.shard_map(local_fn, mesh=mesh, in_specs=(frame_spec, P(), P(), P(), P()), out_specs=frame_spec, check_vma=False)
```
